32 devices in a mesh: cuts: 16 (over z, y, x), site: 2 (over core).
Axes of the slice: x: 2, y: 2, z: 4, core: 2. Of those that a mesh axis runs over, the one named last changes fastest.
Arguments:
- field: float32 [16, 2048], P('cuts'), may hold values from -4 to 4
- momenta: float32 [16, 2048], P('cuts'), may hold values from -4 to 4
- start_force: float32 [16, 2048], P('cuts'), may hold values from -4 to 4
- green: bfloat16 [16, 2048, 2048], P('cuts', 'site'), as said below
- forward_prop: bfloat16 [2048, 2048], P('site')
- back_prop: bfloat16 [2048, 2048], P('site')
- accept: int32 [16], P('cuts'), may hold values from 0 to 1
Outputs:
- new_field: float32 [16, 2048], P('cuts')
- new_momenta: float32 [16, 2048], P('cuts')
- new_force: float32 [16, 2048], P('cuts')
- energy_change: float32 [1], replicated
The draws below stay inside these ranges and needn't reach their ends.
Inputs may be any that keep to these rules, and one draw needn't show every extreme that they name: green has a diagonal of 0.2 to 0.8 plus full-rank off-diagonal entries; the propagators are the identity plus full-rank entries.
All inputs are finite; a program needn't handle non-finite values.
Results may differ from the reference program's by a relative error of at most 0.0029.
Values may be sent and summed in bfloat16 or wider, within the bound.
A program may use at most 128 MiB of HBM per device.

```python
import jax
import jax.numpy as jnp
from jax import lax

N = 2048
SLICES = 16


def draw_green(key, part):
    noise = jax.random.normal(jax.random.fold_in(key, 11), (SLICES, N, N), jnp.float32) * (1.0 / N ** 0.5)
    middle = jax.random.uniform(jax.random.fold_in(key, 12), (SLICES, N, 1), jnp.float32, 0.2, 0.8)
    unit = (jnp.arange(N)[:, None] == jnp.arange(N)[None, :]).astype(jnp.float32)
    return (noise + middle * unit[None, :, :]).astype(jnp.bfloat16)


def propagator(key, salt):
    noise = jax.random.normal(jax.random.fold_in(key, salt), (N, N), jnp.float32) * (1.0 / N ** 0.5)
    unit = (jnp.arange(N)[:, None] == jnp.arange(N)[None, :]).astype(jnp.float32)
    return (noise + unit).astype(jnp.bfloat16)


def draw_forward_prop(key, part):
    return propagator(key, 21)


def draw_back_prop(key, part):
    return propagator(key, 22)


def touch_ends(array, stream_key, smallest, top_value):
    longest = array.shape.index(max(array.shape))
    spots = []
    for shift in (0, 1):
        where = [jax.random.randint(jax.random.fold_in(stream_key, axis), (), 0, length) for axis, length in enumerate(array.shape)]
        where[longest] = (where[longest] + shift) % array.shape[longest]
        spots.append(tuple(where))
    return array.at[spots[0]].set(smallest).at[spots[1]].set(top_value)


def block_scale(rng, dims, cuts, least, high):
    gain, own = 1.0, jax.random.fold_in(rng, 6)
    for dim, blocks in cuts:
        steps = jnp.exp(jax.random.uniform(jax.random.fold_in(own, dim), (blocks,), jnp.float32, least / len(cuts), high / len(cuts)))
        gain = gain * jnp.repeat(steps, dims[dim] // blocks).reshape([-1 if axis == dim else 1 for axis in range(len(dims))])
    return gain


def bell_draw(key, dims, width, reach, cuts=(), kind=jnp.bfloat16):
    loudness = block_scale(key, dims, cuts, -0.22, 0.18) if cuts else 1.0
    values = jax.random.normal(key, dims, jnp.float32) * width * loudness
    return jnp.minimum(jnp.maximum(values, -reach), reach).astype(kind)


def setup_inputs(seed: int = 0) -> dict:
    arg_keys = jax.random.split(jax.random.key(seed), 8)
    field = bell_draw(arg_keys[0], (SLICES, N), 1.0, 4.0, ((0, 16),), jnp.float32)
    momenta = bell_draw(arg_keys[1], (SLICES, N), 1.0, 4.0, ((0, 16),), jnp.float32)
    start_force = bell_draw(arg_keys[2], (SLICES, N), 1.0, 4.0, ((0, 16),), jnp.float32)
    green = draw_green(jax.random.fold_in(arg_keys[7], 71), 0)
    forward_prop = draw_forward_prop(jax.random.fold_in(arg_keys[7], 71), 0)
    back_prop = draw_back_prop(jax.random.fold_in(arg_keys[7], 71), 0)
    accept = touch_ends(jax.random.randint(arg_keys[6], (SLICES,), 0, 2), jax.random.fold_in(arg_keys[6], 1), 0, 1).astype(jnp.int32)
    return {"field": field, "momenta": momenta, "start_force": start_force, "green": green, "forward_prop": forward_prop, "back_prop": back_prop, "accept": accept}


coupling = 0.5
stepsize = 0.2

def reference(field, momenta, start_force, green, forward_prop, back_prop, accept):
    half = momenta - 0.5 * stepsize * start_force
    trial = field + stepsize * half
    previous = jnp.roll(green, 1, axis=0)
    back_wide = back_prop.astype(jnp.float32)

    def one_slice(inputs):
        before, phase = inputs
        scaled = (jnp.exp(coupling * phase)[:, None] * before.astype(jnp.float32)).astype(jnp.bfloat16)
        wrapped = jnp.dot(forward_prop, scaled, preferred_element_type=jnp.float32)
        return lax.optimization_barrier(jnp.sum(wrapped * (jnp.exp(-coupling * phase)[None, :] * back_wide), axis=1))
    diagonal = lax.map(one_slice, (previous, trial))
    new_force = trial - 2.0 * coupling * (1.0 - 2.0 * diagonal)
    new_momenta = half - 0.5 * stepsize * new_force
    total = jnp.sum(new_momenta * new_momenta) + jnp.sum(trial * trial) - jnp.sum(momenta * momenta) - jnp.sum(field * field)
    change = total / (2.0 * jnp.sqrt(jnp.float32(SLICES * N)))
    new_field = jnp.where(accept[:, None] == 1, trial, field)
    return (new_field, new_momenta, new_force, jnp.reshape(change, (1,)).astype(jnp.float32))
```

```python
import functools

import jax
import jax.numpy as jnp
from jax import lax
from jax.experimental import pallas as pl
from jax.experimental.pallas import tpu as pltpu
from jax.sharding import PartitionSpec as P

coupling = 0.5
stepsize = 0.2
LANES = 128
WIDTH = 256
F32 = jnp.float32
MESH = pl.DeviceIdType.MESH


def group_of(slices):
    return max(d for d in range(1, slices + 1) if slices % d == 0 and d * d <= slices)


def half_of(momenta, force):
    return momenta - 0.5 * stepsize * force


def kernel(
    slices, sites, group, count,
    field, momenta, force, green, forward, back, accept,
    new_field, new_momenta, new_force, change,
    own, ahead, mine, other, fwd, bck, grow, shrink, acc, part, diag_out, diag_in, near, far,
    row_sem, load_sem, row_send, row_recv, green_send, green_recv,
    diag_send, diag_recv, near_send, near_recv, far_send, far_recv,
):
    cut = lax.axis_index("cuts")
    site = lax.axis_index("site")
    rows = mine.shape[0]
    size = own.shape[2]
    chunks = green_send.shape[0]
    deep = rows // chunks
    groups = slices // group
    behind = lax.rem(cut + slices - 1, slices)
    after = lax.rem(cut + 1, slices)
    base = (cut // group) * group
    spot = lax.rem(cut, group)
    block = cut // group
    slot = spot * sites + site

    near_peers = []
    for step in range(1, group * sites):
        peer = lax.rem(slot + step, group * sites)
        near_peers.append((peer, {"cuts": base + peer // sites, "site": lax.rem(peer, sites)}))
    far_peers = []
    for step in range(1, groups):
        peer = lax.rem(block + step, groups)
        far_peers.append((peer, {"cuts": peer * group + spot, "site": site}))
    partner = {"cuts": cut, "site": 1 - site}

    barrier = pltpu.get_barrier_semaphore()
    greet = [p for _, p in near_peers] + [p for _, p in far_peers]
    greet += [{"cuts": c, "site": s} for c in (behind, after) for s in range(sites)]
    for p in greet:
        pl.semaphore_signal(barrier, inc=1, device_id=p, device_id_type=MESH)

    row_loads = [
        pltpu.make_async_copy(src, own.at[i], row_sem.at[i])
        for i, src in enumerate((field, momenta, force))
    ]
    for c in row_loads:
        c.start()
    green_loads = [
        pltpu.make_async_copy(
            green.at[0, pl.ds(i * deep, deep)], mine.at[pl.ds(i * deep, deep)], load_sem.at[i]
        )
        for i in range(chunks)
    ]
    for c in green_loads:
        c.start()
    fwd_loads = [
        pltpu.make_async_copy(
            forward.at[:, pl.ds(pl.multiple_of(k * rows, LANES), rows)],
            fwd.at[i],
            load_sem.at[chunks + i],
        )
        for i, k in enumerate((site, 1 - site))
    ]
    back_load = pltpu.make_async_copy(back, bck, load_sem.at[chunks + 2])
    fwd_loads[0].start()
    back_load.start()
    fwd_loads[1].start()

    for c in row_loads:
        c.wait()
    pl.semaphore_wait(barrier, len(greet))

    row_sends = [
        pltpu.make_async_remote_copy(
            own.at[i], ahead.at[i], row_send.at[i], row_recv.at[i],
            device_id={"cuts": behind, "site": site}, device_id_type=MESH,
        )
        for i in range(3)
    ]
    for c in row_sends:
        c.start()
    green_sends = [
        pltpu.make_async_remote_copy(
            mine.at[pl.ds(i * deep, deep)], other.at[pl.ds(i * deep, deep)],
            green_send.at[i], green_recv.at[i],
            device_id=partner, device_id_type=MESH,
        )
        for i in range(chunks)
    ]
    for load, send in zip(green_loads, green_sends):
        load.wait()
        send.start()

    half = half_of(own[1], own[2])
    trial = own[0] + stepsize * half
    new_field[...] = jnp.where(accept[0] == 1, trial, own[0])

    for c in row_sends:
        c.wait_recv()
    phase = ahead[0] + stepsize * half_of(ahead[1], ahead[2])
    shrink[...] = jnp.exp(-coupling * phase)
    ahead_rows = pl.ds(pl.multiple_of(site * rows, LANES), rows)
    other_rows = pl.ds(pl.multiple_of((1 - site) * rows, LANES), rows)
    for h, where in enumerate((ahead_rows, other_rows)):
        line = ahead[0, :, where] + stepsize * half_of(ahead[1, :, where], ahead[2, :, where])
        line = jnp.exp(coupling * line)
        for b in range(rows // LANES):
            tile = jnp.broadcast_to(line[:, b * LANES:(b + 1) * LANES], (LANES, LANES))
            grow[h, b * LANES:(b + 1) * LANES, :] = tile.T
    part[...] = jnp.zeros_like(part)

    def product(h, source, columns):
        g = source[:, columns].astype(F32)
        e = grow[h]
        scaled = jnp.concatenate(
            [
                (e * g[:, i:i + LANES]).astype(jnp.bfloat16)
                for i in range(0, WIDTH, LANES)
            ],
            axis=1,
        )
        return jnp.dot(fwd[h], scaled, preferred_element_type=F32)

    fwd_loads[0].wait()

    @pl.loop(0, size // WIDTH)
    def _(j):
        columns = pl.ds(pl.multiple_of(j * WIDTH, WIDTH), WIDTH)
        acc[:, columns] = product(0, mine, columns)

    back_load.wait()
    fwd_loads[1].wait()
    for c in green_sends:
        c.wait_recv()

    @pl.loop(0, size // WIDTH)
    def _(j):
        columns = pl.ds(pl.multiple_of(j * WIDTH, WIDTH), WIDTH)
        wrapped = acc[:, columns] + product(1, other, columns)
        terms = wrapped * (shrink[:, columns] * bck[:, columns].astype(F32))
        total = part[...]
        for i in range(0, WIDTH, LANES):
            total = total + terms[:, i:i + LANES]
        part[...] = total

    line = jnp.concatenate(
        [
            jnp.sum(part[b * LANES:(b + 1) * LANES, :].T, axis=0, keepdims=True)
            for b in range(rows // LANES)
        ],
        axis=1,
    )
    diag_out[...] = line
    diag_sends = [
        pltpu.make_async_remote_copy(
            diag_out, diag_in.at[site], diag_send.at[s], diag_recv.at[site],
            device_id={"cuts": after, "site": s}, device_id_type=MESH,
        )
        for s in range(sites)
    ]
    for c in diag_sends:
        c.start()

    f, m = ahead[0, :, ahead_rows], ahead[1, :, ahead_rows]
    h = half_of(m, ahead[2, :, ahead_rows])
    t = f + stepsize * h
    n = h - 0.5 * stepsize * (t - 2.0 * coupling * (1.0 - 2.0 * line))
    energy = (n * n - m * m) + (t * t - f * f)
    lump = energy[:, :LANES]
    for i in range(LANES, rows, LANES):
        lump = lump + energy[:, i:i + LANES]
    near[slot] = lump
    near_sends = [
        pltpu.make_async_remote_copy(
            near.at[slot], near.at[slot], near_send.at[i], near_recv.at[slot],
            device_id=p, device_id_type=MESH,
        )
        for i, (_, p) in enumerate(near_peers)
    ]
    for c in near_sends:
        c.start()
    for peer, _ in near_peers:
        pltpu.make_async_copy(near.at[peer], near.at[peer], near_recv.at[peer]).wait()
    lump = near[0]
    for i in range(1, group * sites):
        lump = lump + near[i]
    far[block] = lump
    far_sends = [
        pltpu.make_async_remote_copy(
            far.at[block], far.at[block], far_send.at[i], far_recv.at[block],
            device_id=p, device_id_type=MESH,
        )
        for i, (_, p) in enumerate(far_peers)
    ]
    for c in far_sends:
        c.start()

    for s in range(sites):
        pltpu.make_async_copy(diag_in.at[s], diag_in.at[s], diag_recv.at[s]).wait()
    diagonal = jnp.concatenate([diag_in[s] for s in range(sites)], axis=1)
    force_now = trial - 2.0 * coupling * (1.0 - 2.0 * diagonal)
    new_force[...] = force_now
    new_momenta[...] = half - 0.5 * stepsize * force_now

    for peer, _ in far_peers:
        pltpu.make_async_copy(far.at[peer], far.at[peer], far_recv.at[peer]).wait()
    lump = far[0]
    for i in range(1, groups):
        lump = lump + far[i]
    change[0] = jnp.sum(lump) * (1.0 / (2.0 * count ** 0.5))

    for c in row_sends + green_sends + diag_sends + near_sends + far_sends:
        c.wait_send()


def on_device(slices, sites, field, momenta, start_force, green, forward_prop, back_prop, accept):
    size = field.shape[1]
    rows = green.shape[1]
    group = group_of(slices)
    groups = slices // group
    chunks = 4
    row = jax.ShapeDtypeStruct(field.shape, F32)
    bf = jnp.bfloat16
    dma = pltpu.SemaphoreType.DMA
    any_space = pl.BlockSpec(memory_space=pl.ANY)
    vmem = pl.BlockSpec(memory_space=pltpu.VMEM)
    smem = pl.BlockSpec(memory_space=pltpu.SMEM)
    return pl.pallas_call(
        functools.partial(kernel, slices, sites, group, slices * field.shape[0] * size),
        out_shape=(row, row, row, jax.ShapeDtypeStruct((1,), F32)),
        in_specs=[any_space] * 6 + [smem],
        out_specs=(vmem, vmem, vmem, smem),
        scratch_shapes=[
            pltpu.VMEM((3, 1, size), F32),
            pltpu.VMEM((3, 1, size), F32),
            pltpu.VMEM((rows, size), bf),
            pltpu.VMEM((rows, size), bf),
            pltpu.VMEM((2, rows, rows), bf),
            pltpu.VMEM((rows, size), bf),
            pltpu.VMEM((2, rows, LANES), F32),
            pltpu.VMEM((1, size), F32),
            pltpu.VMEM((rows, size), F32),
            pltpu.VMEM((rows, LANES), F32),
            pltpu.VMEM((1, rows), F32),
            pltpu.VMEM((sites, 1, rows), F32),
            pltpu.VMEM((group * sites, 1, LANES), F32),
            pltpu.VMEM((groups, 1, LANES), F32),
            dma((3,)), dma((chunks + 3,)),
            dma((3,)), dma((3,)),
            dma((chunks,)), dma((chunks,)),
            dma((sites,)), dma((sites,)),
            dma((group * sites,)), dma((group * sites,)),
            dma((groups,)), dma((groups,)),
        ],
        compiler_params=pltpu.CompilerParams(
            collective_id=0, has_side_effects=True, vmem_limit_bytes=60 * 1024 * 1024
        ),
        name="leapfrog",
    )(field, momenta, start_force, green, forward_prop, back_prop, accept)


def solution(mesh):
    return jax.shard_map(
        functools.partial(on_device, mesh.shape["cuts"], mesh.shape["site"]),
        mesh=mesh,
        in_specs=(
            P("cuts", None),
            P("cuts", None),
            P("cuts", None),
            P("cuts", "site", None),
            P("site", None),
            P("site", None),
            P("cuts"),
        ),
        out_specs=(P("cuts", None), P("cuts", None), P("cuts", None), P()),
        check_vma=False,
    )
```

```python
import functools

import jax
import jax.numpy as jnp
from jax import lax
from jax.experimental import pallas as pl
from jax.experimental.pallas import tpu as pltpu
from jax.sharding import PartitionSpec as P

coupling = 0.5
stepsize = 0.2
LANES = 128
WIDTH = 256
F32 = jnp.float32
MESH = pl.DeviceIdType.MESH


def group_of(slices, sites):
    return max(d for d in range(1, slices + 1) if slices % d == 0 and d * sites <= 32)


def half_of(momenta, force):
    return momenta - 0.5 * stepsize * force


def kernel(
    slices, sites, group,
    field, momenta, force, green, forward, back,
    packed,
    own, ahead, mine, other, fwd, bck, grow, shrink, acc, part, diag_out, diag_in, near, far,
    row_sem, load_sem, row_send, row_recv, green_send, green_recv,
    diag_send, diag_recv, near_send, near_recv, far_send, far_recv,
):
    cut = lax.axis_index("cuts")
    site = lax.axis_index("site")
    rows = mine.shape[0]
    size = own.shape[2]
    chunks = green_send.shape[0]
    deep = rows // chunks
    groups = slices // group
    behind = lax.rem(cut + slices - 1, slices)
    after = lax.rem(cut + 1, slices)
    base = (cut // group) * group
    spot = lax.rem(cut, group)
    block = cut // group
    slot = spot * sites + site

    near_peers = []
    for step in range(1, group * sites):
        peer = lax.rem(slot + step, group * sites)
        near_peers.append((peer, {"cuts": base + peer // sites, "site": lax.rem(peer, sites)}))
    far_peers = []
    for step in range(1, groups):
        peer = lax.rem(block + step, groups)
        far_peers.append((peer, {"cuts": peer * group + spot, "site": site}))
    partner = {"cuts": cut, "site": 1 - site}

    barrier = pltpu.get_barrier_semaphore()
    greet = [p for _, p in near_peers] + [p for _, p in far_peers]
    greet += [{"cuts": c, "site": s} for c in (behind, after) for s in range(sites)]
    for p in greet:
        pl.semaphore_signal(barrier, inc=1, device_id=p, device_id_type=MESH)

    row_loads = [
        pltpu.make_async_copy(src, own.at[i], row_sem.at[i])
        for i, src in enumerate((field, momenta, force))
    ]
    for c in row_loads:
        c.start()
    green_loads = [
        pltpu.make_async_copy(
            green.at[0, pl.ds(i * deep, deep)], mine.at[pl.ds(i * deep, deep)], load_sem.at[i]
        )
        for i in range(chunks)
    ]
    for c in green_loads:
        c.start()
    fwd_loads = [
        pltpu.make_async_copy(
            forward.at[:, pl.ds(pl.multiple_of(k * rows, LANES), rows)],
            fwd.at[i],
            load_sem.at[chunks + i],
        )
        for i, k in enumerate((site, 1 - site))
    ]
    back_load = pltpu.make_async_copy(back, bck, load_sem.at[chunks + 2])
    fwd_loads[0].start()
    back_load.start()
    fwd_loads[1].start()

    for c in row_loads:
        c.wait()
    pl.semaphore_wait(barrier, len(greet))

    row_sends = [
        pltpu.make_async_remote_copy(
            own.at[i], ahead.at[i], row_send.at[i], row_recv.at[i],
            device_id={"cuts": behind, "site": site}, device_id_type=MESH,
        )
        for i in range(3)
    ]
    for c in row_sends:
        c.start()
    green_sends = [
        pltpu.make_async_remote_copy(
            mine.at[pl.ds(i * deep, deep)], other.at[pl.ds(i * deep, deep)],
            green_send.at[i], green_recv.at[i],
            device_id=partner, device_id_type=MESH,
        )
        for i in range(chunks)
    ]
    for load, send in zip(green_loads, green_sends):
        load.wait()
        send.start()

    half = half_of(own[1], own[2])
    trial = own[0] + stepsize * half
    packed[:, :size] = trial

    for c in row_sends:
        c.wait_recv()
    phase = ahead[0] + stepsize * half_of(ahead[1], ahead[2])
    shrink[...] = jnp.exp(-coupling * phase)
    ahead_rows = pl.ds(pl.multiple_of(site * rows, LANES), rows)
    other_rows = pl.ds(pl.multiple_of((1 - site) * rows, LANES), rows)
    for h, where in enumerate((ahead_rows, other_rows)):
        line = ahead[0, :, where] + stepsize * half_of(ahead[1, :, where], ahead[2, :, where])
        line = jnp.exp(coupling * line)
        for b in range(rows // LANES):
            tile = jnp.broadcast_to(line[:, b * LANES:(b + 1) * LANES], (LANES, LANES))
            grow[h, b * LANES:(b + 1) * LANES, :] = tile.T
    part[...] = jnp.zeros_like(part)

    def product(h, source, columns):
        g = source[:, columns].astype(F32)
        e = grow[h]
        scaled = jnp.concatenate(
            [
                (e * g[:, i:i + LANES]).astype(jnp.bfloat16)
                for i in range(0, WIDTH, LANES)
            ],
            axis=1,
        )
        return jnp.dot(fwd[h], scaled, preferred_element_type=F32)

    fwd_loads[0].wait()

    @pl.loop(0, size // WIDTH)
    def _(j):
        columns = pl.ds(pl.multiple_of(j * WIDTH, WIDTH), WIDTH)
        acc[:, columns] = product(0, mine, columns)

    back_load.wait()
    fwd_loads[1].wait()
    for c in green_sends:
        c.wait_recv()

    @pl.loop(0, size // WIDTH)
    def _(j):
        columns = pl.ds(pl.multiple_of(j * WIDTH, WIDTH), WIDTH)
        wrapped = acc[:, columns] + product(1, other, columns)
        terms = wrapped * (shrink[:, columns] * bck[:, columns].astype(F32))
        total = part[...]
        for i in range(0, WIDTH, LANES):
            total = total + terms[:, i:i + LANES]
        part[...] = total

    line = jnp.concatenate(
        [
            jnp.sum(part[b * LANES:(b + 1) * LANES, :].T, axis=0, keepdims=True)
            for b in range(rows // LANES)
        ],
        axis=1,
    )
    diag_out[...] = line
    diag_sends = [
        pltpu.make_async_remote_copy(
            diag_out, diag_in.at[site], diag_send.at[s], diag_recv.at[site],
            device_id={"cuts": after, "site": s}, device_id_type=MESH,
        )
        for s in range(sites)
    ]
    for c in diag_sends:
        c.start()

    f, m = ahead[0, :, ahead_rows], ahead[1, :, ahead_rows]
    h = half_of(m, ahead[2, :, ahead_rows])
    t = f + stepsize * h
    n = h - 0.5 * stepsize * (t - 2.0 * coupling * (1.0 - 2.0 * line))
    energy = (n * n - m * m) + (t * t - f * f)
    lump = energy[:, :LANES]
    for i in range(LANES, rows, LANES):
        lump = lump + energy[:, i:i + LANES]
    near[slot] = lump
    near_sends = [
        pltpu.make_async_remote_copy(
            near.at[slot], near.at[slot], near_send.at[i], near_recv.at[slot],
            device_id=p, device_id_type=MESH,
        )
        for i, (_, p) in enumerate(near_peers)
    ]
    for c in near_sends:
        c.start()
    for peer, _ in near_peers:
        pltpu.make_async_copy(near.at[peer], near.at[peer], near_recv.at[peer]).wait()
    lump = near[0]
    for i in range(1, group * sites):
        lump = lump + near[i]
    far[block] = lump
    far_sends = [
        pltpu.make_async_remote_copy(
            far.at[block], far.at[block], far_send.at[i], far_recv.at[block],
            device_id=p, device_id_type=MESH,
        )
        for i, (_, p) in enumerate(far_peers)
    ]
    for c in far_sends:
        c.start()

    for s in range(sites):
        pltpu.make_async_copy(diag_in.at[s], diag_in.at[s], diag_recv.at[s]).wait()
    diagonal = jnp.concatenate([diag_in[s] for s in range(sites)], axis=1)
    force_now = trial - 2.0 * coupling * (1.0 - 2.0 * diagonal)
    packed[:, size:2 * size] = half - 0.5 * stepsize * force_now
    packed[:, 2 * size:3 * size] = force_now

    for peer, _ in far_peers:
        pltpu.make_async_copy(far.at[peer], far.at[peer], far_recv.at[peer]).wait()
    lump = far[0]
    for i in range(1, groups):
        lump = lump + far[i]
    packed[:, 3 * size:] = lump

    for c in row_sends + green_sends + diag_sends + near_sends + far_sends:
        c.wait_send()


def split(count, packed, field, accept, new_field, new_momenta, new_force, change):
    size = new_field.shape[1]
    taken = accept[0]
    new_field[...] = jnp.where(taken == 1, packed[:, :size], field[...])
    new_momenta[...] = packed[:, size:2 * size]
    new_force[...] = packed[:, 2 * size:3 * size]
    change[0] = jnp.sum(packed[:, 3 * size:]) * (1.0 / (2.0 * count ** 0.5))


def on_device(slices, sites, field, momenta, start_force, green, forward_prop, back_prop, accept):
    size = field.shape[1]
    rows = green.shape[1]
    group = group_of(slices, sites)
    groups = slices // group
    chunks = 4
    row = jax.ShapeDtypeStruct(field.shape, F32)
    bf = jnp.bfloat16
    dma = pltpu.SemaphoreType.DMA
    any_space = pl.BlockSpec(memory_space=pl.ANY)
    vmem = pl.BlockSpec(memory_space=pltpu.VMEM)
    smem = pl.BlockSpec(memory_space=pltpu.SMEM)
    packed = pl.pallas_call(
        functools.partial(kernel, slices, sites, group),
        out_shape=jax.ShapeDtypeStruct((1, 3 * size + LANES), F32),
        in_specs=[any_space] * 6,
        out_specs=vmem,
        scratch_shapes=[
            pltpu.VMEM((3, 1, size), F32),
            pltpu.VMEM((3, 1, size), F32),
            pltpu.VMEM((rows, size), bf),
            pltpu.VMEM((rows, size), bf),
            pltpu.VMEM((2, rows, rows), bf),
            pltpu.VMEM((rows, size), bf),
            pltpu.VMEM((2, rows, LANES), F32),
            pltpu.VMEM((1, size), F32),
            pltpu.VMEM((rows, size), F32),
            pltpu.VMEM((rows, LANES), F32),
            pltpu.VMEM((1, rows), F32),
            pltpu.VMEM((sites, 1, rows), F32),
            pltpu.VMEM((group * sites, 1, LANES), F32),
            pltpu.VMEM((groups, 1, LANES), F32),
            dma((3,)), dma((chunks + 3,)),
            dma((3,)), dma((3,)),
            dma((chunks,)), dma((chunks,)),
            dma((sites,)), dma((sites,)),
            dma((group * sites,)), dma((group * sites,)),
            dma((groups,)), dma((groups,)),
        ],
        compiler_params=pltpu.CompilerParams(
            collective_id=0, has_side_effects=True, vmem_limit_bytes=60 * 1024 * 1024
        ),
        name="leapfrog",
    )(field, momenta, start_force, green, forward_prop, back_prop)
    return pl.pallas_call(
        functools.partial(split, slices * field.shape[0] * size),
        out_shape=(row, row, row, jax.ShapeDtypeStruct((1,), F32)),
        in_specs=[vmem, vmem, smem],
        out_specs=(vmem, vmem, vmem, smem),
        name="split",
    )(packed, field, accept)


def solution(mesh):
    return jax.shard_map(
        functools.partial(on_device, mesh.shape["cuts"], mesh.shape["site"]),
        mesh=mesh,
        in_specs=(
            P("cuts", None),
            P("cuts", None),
            P("cuts", None),
            P("cuts", "site", None),
            P("site", None),
            P("site", None),
            P("cuts"),
        ),
        out_specs=(P("cuts", None), P("cuts", None), P("cuts", None), P()),
        check_vma=False,
    )
```

```python
import functools

import jax
import jax.numpy as jnp
from jax import lax
from jax.experimental import pallas as pl
from jax.experimental.pallas import tpu as pltpu
from jax.sharding import PartitionSpec as P

coupling = 0.5
stepsize = 0.2
LANES = 128
WIDTH = 256
F32 = jnp.float32
MESH = pl.DeviceIdType.MESH


def group_of(slices, sites):
    return max(d for d in range(1, slices + 1) if slices % d == 0 and d * sites <= 32)


def half_of(momenta, force):
    return momenta - 0.5 * stepsize * force


def kernel(
    slices, sites, group,
    field, momenta, force, green, forward, back,
    packed,
    own, ahead, mine, other, fwd, bck, grow, shrink, acc, part, diag_out, diag_in, near, far,
    row_sem, load_sem, row_send, row_recv, green_send, green_recv,
    diag_send, diag_recv, near_send, near_recv, far_send, far_recv,
):
    cut = lax.axis_index("cuts")
    site = lax.axis_index("site")
    rows = mine.shape[0]
    size = own.shape[2]
    chunks = green_send.shape[0]
    deep = rows // chunks
    groups = slices // group
    behind = lax.rem(cut + slices - 1, slices)
    after = lax.rem(cut + 1, slices)
    base = (cut // group) * group
    spot = lax.rem(cut, group)
    block = cut // group
    slot = spot * sites + site

    near_peers = []
    for step in range(1, group * sites):
        peer = lax.rem(slot + step, group * sites)
        near_peers.append((peer, {"cuts": base + peer // sites, "site": lax.rem(peer, sites)}))
    far_peers = []
    for step in range(1, groups):
        peer = lax.rem(block + step, groups)
        far_peers.append((peer, {"cuts": peer * group + spot, "site": site}))
    partner = {"cuts": cut, "site": 1 - site}

    barrier = pltpu.get_barrier_semaphore()
    greet = [p for _, p in near_peers] + [p for _, p in far_peers]
    greet += [{"cuts": c, "site": s} for c in (behind, after) for s in range(sites)]
    for p in greet:
        pl.semaphore_signal(barrier, inc=1, device_id=p, device_id_type=MESH)

    row_loads = [
        pltpu.make_async_copy(src, own.at[i], row_sem.at[i])
        for i, src in enumerate((field, momenta, force))
    ]
    for c in row_loads:
        c.start()
    green_loads = [
        pltpu.make_async_copy(
            green.at[0, pl.ds(i * deep, deep)], mine.at[pl.ds(i * deep, deep)], load_sem.at[i]
        )
        for i in range(chunks)
    ]
    for c in green_loads:
        c.start()
    fwd_loads = [
        pltpu.make_async_copy(
            forward.at[:, pl.ds(pl.multiple_of(k * rows, LANES), rows)],
            fwd.at[i],
            load_sem.at[chunks + i],
        )
        for i, k in enumerate((site, 1 - site))
    ]
    back_load = pltpu.make_async_copy(back, bck, load_sem.at[chunks + 2])
    fwd_loads[0].start()
    back_load.start()
    fwd_loads[1].start()

    for c in row_loads:
        c.wait()
    pl.semaphore_wait(barrier, len(greet))

    row_sends = [
        pltpu.make_async_remote_copy(
            own.at[i], ahead.at[i], row_send.at[3 * s + i], row_recv.at[i],
            device_id={"cuts": behind, "site": s}, device_id_type=MESH,
        )
        for s in range(sites) for i in range(3)
    ]

    @pl.when(site == sites - 1)
    def _():
        for c in row_sends:
            c.start()

    green_sends = [
        pltpu.make_async_remote_copy(
            mine.at[pl.ds(i * deep, deep)], other.at[pl.ds(i * deep, deep)],
            green_send.at[i], green_recv.at[i],
            device_id=partner, device_id_type=MESH,
        )
        for i in range(chunks)
    ]
    for load, send in zip(green_loads, green_sends):
        load.wait()
        send.start()

    half = half_of(own[1], own[2])
    trial = own[0] + stepsize * half
    packed[:, :size] = trial

    for i in range(3):
        pltpu.make_async_copy(ahead.at[i], ahead.at[i], row_recv.at[i]).wait()
    phase = ahead[0] + stepsize * half_of(ahead[1], ahead[2])
    shrink[...] = jnp.exp(-coupling * phase)
    ahead_rows = pl.ds(pl.multiple_of(site * rows, LANES), rows)
    other_rows = pl.ds(pl.multiple_of((1 - site) * rows, LANES), rows)
    for h, where in enumerate((ahead_rows, other_rows)):
        line = ahead[0, :, where] + stepsize * half_of(ahead[1, :, where], ahead[2, :, where])
        line = jnp.exp(coupling * line)
        for b in range(rows // LANES):
            tile = jnp.broadcast_to(line[:, b * LANES:(b + 1) * LANES], (LANES, LANES))
            grow[h, b * LANES:(b + 1) * LANES, :] = tile.T
    part[...] = jnp.zeros_like(part)

    def product(h, source, columns):
        g = source[:, columns].astype(F32)
        e = grow[h]
        scaled = jnp.concatenate(
            [
                (e * g[:, i:i + LANES]).astype(jnp.bfloat16)
                for i in range(0, WIDTH, LANES)
            ],
            axis=1,
        )
        return jnp.dot(fwd[h], scaled, preferred_element_type=F32)

    fwd_loads[0].wait()

    @pl.loop(0, size // WIDTH)
    def _(j):
        columns = pl.ds(pl.multiple_of(j * WIDTH, WIDTH), WIDTH)
        acc[:, columns] = product(0, mine, columns)

    back_load.wait()
    fwd_loads[1].wait()
    for c in green_sends:
        c.wait_recv()

    @pl.loop(0, size // WIDTH)
    def _(j):
        columns = pl.ds(pl.multiple_of(j * WIDTH, WIDTH), WIDTH)
        wrapped = acc[:, columns] + product(1, other, columns)
        terms = wrapped * (shrink[:, columns] * bck[:, columns].astype(F32))
        total = part[...]
        for i in range(0, WIDTH, LANES):
            total = total + terms[:, i:i + LANES]
        part[...] = total

    line = jnp.concatenate(
        [
            jnp.sum(part[b * LANES:(b + 1) * LANES, :].T, axis=0, keepdims=True)
            for b in range(rows // LANES)
        ],
        axis=1,
    )
    diag_out[...] = line
    diag_sends = [
        pltpu.make_async_remote_copy(
            diag_out, diag_in.at[site], diag_send.at[s], diag_recv.at[site],
            device_id={"cuts": after, "site": s}, device_id_type=MESH,
        )
        for s in range(sites)
    ]
    for c in diag_sends:
        c.start()

    f, m = ahead[0, :, ahead_rows], ahead[1, :, ahead_rows]
    h = half_of(m, ahead[2, :, ahead_rows])
    t = f + stepsize * h
    n = h - 0.5 * stepsize * (t - 2.0 * coupling * (1.0 - 2.0 * line))
    energy = (n * n - m * m) + (t * t - f * f)
    lump = energy[:, :LANES]
    for i in range(LANES, rows, LANES):
        lump = lump + energy[:, i:i + LANES]
    near[slot] = lump
    near_sends = [
        pltpu.make_async_remote_copy(
            near.at[slot], near.at[slot], near_send.at[i], near_recv.at[slot],
            device_id=p, device_id_type=MESH,
        )
        for i, (_, p) in enumerate(near_peers)
    ]
    for c in near_sends:
        c.start()
    for peer, _ in near_peers:
        pltpu.make_async_copy(near.at[peer], near.at[peer], near_recv.at[peer]).wait()
    lump = near[0]
    for i in range(1, group * sites):
        lump = lump + near[i]
    far[block] = lump
    far_sends = [
        pltpu.make_async_remote_copy(
            far.at[block], far.at[block], far_send.at[i], far_recv.at[block],
            device_id=p, device_id_type=MESH,
        )
        for i, (_, p) in enumerate(far_peers)
    ]
    for c in far_sends:
        c.start()

    for s in range(sites):
        pltpu.make_async_copy(diag_in.at[s], diag_in.at[s], diag_recv.at[s]).wait()
    diagonal = jnp.concatenate([diag_in[s] for s in range(sites)], axis=1)
    force_now = trial - 2.0 * coupling * (1.0 - 2.0 * diagonal)
    packed[:, size:2 * size] = half - 0.5 * stepsize * force_now
    packed[:, 2 * size:3 * size] = force_now

    for peer, _ in far_peers:
        pltpu.make_async_copy(far.at[peer], far.at[peer], far_recv.at[peer]).wait()
    lump = far[0]
    for i in range(1, groups):
        lump = lump + far[i]
    packed[:, 3 * size:] = lump

    @pl.when(site == sites - 1)
    def _():
        for c in row_sends:
            c.wait_send()

    for c in green_sends + diag_sends + near_sends + far_sends:
        c.wait_send()


def split(count, packed, field, accept, new_field, new_momenta, new_force, change):
    size = new_field.shape[1]
    taken = accept[0]
    new_field[...] = jnp.where(taken == 1, packed[:, :size], field[...])
    new_momenta[...] = packed[:, size:2 * size]
    new_force[...] = packed[:, 2 * size:3 * size]
    change[0] = jnp.sum(packed[:, 3 * size:]) * (1.0 / (2.0 * count ** 0.5))


def on_device(slices, sites, field, momenta, start_force, green, forward_prop, back_prop, accept):
    size = field.shape[1]
    rows = green.shape[1]
    group = group_of(slices, sites)
    groups = slices // group
    chunks = 4
    row = jax.ShapeDtypeStruct(field.shape, F32)
    bf = jnp.bfloat16
    dma = pltpu.SemaphoreType.DMA
    any_space = pl.BlockSpec(memory_space=pl.ANY)
    vmem = pl.BlockSpec(memory_space=pltpu.VMEM)
    smem = pl.BlockSpec(memory_space=pltpu.SMEM)
    packed = pl.pallas_call(
        functools.partial(kernel, slices, sites, group),
        out_shape=jax.ShapeDtypeStruct((1, 3 * size + LANES), F32),
        in_specs=[any_space] * 6,
        out_specs=vmem,
        scratch_shapes=[
            pltpu.VMEM((3, 1, size), F32),
            pltpu.VMEM((3, 1, size), F32),
            pltpu.VMEM((rows, size), bf),
            pltpu.VMEM((rows, size), bf),
            pltpu.VMEM((2, rows, rows), bf),
            pltpu.VMEM((rows, size), bf),
            pltpu.VMEM((2, rows, LANES), F32),
            pltpu.VMEM((1, size), F32),
            pltpu.VMEM((rows, size), F32),
            pltpu.VMEM((rows, LANES), F32),
            pltpu.VMEM((1, rows), F32),
            pltpu.VMEM((sites, 1, rows), F32),
            pltpu.VMEM((group * sites, 1, LANES), F32),
            pltpu.VMEM((groups, 1, LANES), F32),
            dma((3,)), dma((chunks + 3,)),
            dma((3 * sites,)), dma((3,)),
            dma((chunks,)), dma((chunks,)),
            dma((sites,)), dma((sites,)),
            dma((group * sites,)), dma((group * sites,)),
            dma((groups,)), dma((groups,)),
        ],
        compiler_params=pltpu.CompilerParams(
            collective_id=0, has_side_effects=True, vmem_limit_bytes=60 * 1024 * 1024
        ),
        name="leapfrog",
    )(field, momenta, start_force, green, forward_prop, back_prop)
    return pl.pallas_call(
        functools.partial(split, slices * field.shape[0] * size),
        out_shape=(row, row, row, jax.ShapeDtypeStruct((1,), F32)),
        in_specs=[vmem, vmem, smem],
        out_specs=(vmem, vmem, vmem, smem),
        name="split",
    )(packed, field, accept)


def solution(mesh):
    return jax.shard_map(
        functools.partial(on_device, mesh.shape["cuts"], mesh.shape["site"]),
        mesh=mesh,
        in_specs=(
            P("cuts", None),
            P("cuts", None),
            P("cuts", None),
            P("cuts", "site", None),
            P("site", None),
            P("site", None),
            P("cuts"),
        ),
        out_specs=(P("cuts", None), P("cuts", None), P("cuts", None), P()),
        check_vma=False,
    )
```
